256 devices in a mesh: row: 16 (over z_hi, y), col: 16 (over z_lo, x, core).
Axes of the slice: x: 4, y: 4, z: 8 (z_hi: 4, z_lo: 2; z = z_hi * 2 + z_lo), core: 2. Of those that a mesh axis runs over, the one named last changes fastest.
Arguments:
- tokens: bfloat16 [8192, 4096], P('row', 'col'), may hold values from -6 to 6
- norm_gain: bfloat16 [4096], P('col'), may hold values from 0.099609375 to 1.8984375
- gate_weight: bfloat16 [4096, 10240], P('row', 'col'), may hold values from -0.09375 to 0.09375
- linear_weight: bfloat16 [4096, 10240], P('row', 'col'), may hold values from -0.09375 to 0.09375
- output_weight: bfloat16 [10240, 4096], P('col', 'row'), may hold values from -0.078125 to 0.078125
Outputs:
- block_out: bfloat16 [8192, 4096], P('row', 'col')
The draws below stay inside these ranges and needn't reach their ends.
All inputs are finite; a program needn't handle non-finite values.
Results may differ from the reference program's by a relative error of at most 0.0065.
Values may be sent and summed in bfloat16 or wider, within the bound.
No kernel may reach another device: no remote copies, remote signals or barrier semaphores. Data moves between devices by JAX's collectives and lax.ppermute only.
A program may use at most 128 MiB of HBM per device.

```python
import jax
import jax.numpy as jnp
from jax import lax

D = 4096
FF = 10240
TOKENS = 8192


def raised(entries, key, source, target, shards_of, factor):
    owner, partner = [(jnp.arange(entries.shape[dim]) // (entries.shape[dim] // shards_of)).reshape([-1 if axis == dim else 1 for axis in range(entries.ndim)]) for dim in (source, target)]
    chosen = jax.random.permutation(key, shards_of)[partner]
    strong = (owner == chosen) | (owner == (partner + shards_of // 2) % shards_of)
    return jnp.where(strong, factor * entries, entries)


def steps_of(key, dims, pieces, low, high):
    def one(axis_at, shards_of):
        heights = jax.random.uniform(jax.random.fold_in(jax.random.fold_in(key, 6), axis_at), (shards_of,), jnp.float32, low / len(pieces), high / len(pieces))
        return jnp.repeat(jnp.exp(heights), dims[axis_at] // shards_of).reshape((-1,) + (1,) * (len(dims) - axis_at - 1))

    gain = one(*pieces[0])
    for cut in pieces[1:]:
        gain = gain * one(*cut)
    return gain


def scatter_about(key, shape, deviation, reach, pieces=(), dtype=jnp.bfloat16):
    array = deviation * jax.random.normal(key, shape, jnp.float32)
    if pieces:
        array = array * steps_of(key, shape, pieces, -0.22, 0.18)
    return jnp.clip(array, -reach, reach).astype(dtype)


def noise_with(rng, dims, width, bound, pieces, heavy, kind=jnp.bfloat16):
    result = width * jax.random.normal(rng, dims, jnp.float32)
    if pieces:
        result = result * steps_of(rng, dims, pieces, -0.22, 0.18)
    return jnp.clip(raised(result, jax.random.fold_in(rng, 3), *heavy), -bound, bound).astype(kind)


def setup_inputs(seed: int = 0) -> dict:
    key_of = jax.random.split(jax.random.key(seed), 6)
    return {
        "tokens": scatter_about(key_of[0], (TOKENS, D), 1.0, 6.0, ((0, 16), (1, 16))),
        "norm_gain": jnp.clip(1.0 + 0.18 * jax.random.normal(key_of[1], (D,), jnp.float32), 0.099609375, 1.8984375).astype(jnp.bfloat16),
        "gate_weight": scatter_about(key_of[2], (D, FF), D ** -0.5, 0.09375, ((0, 16), (1, 16))),
        "linear_weight": scatter_about(key_of[3], (D, FF), D ** -0.5, 0.09375, ((0, 16), (1, 16))),
        "output_weight": noise_with(key_of[4], (FF, D), FF ** -0.5, 0.078125, ((0, 16), (1, 16)), (0, 1, 16, 2.0)),
    }


def reference(tokens, norm_gain, gate_weight, linear_weight, output_weight):
    values = tokens.astype(jnp.float32)
    meansq = lax.optimization_barrier(jnp.mean(values * values, axis=-1, keepdims=True))
    normed = (values * jax.lax.rsqrt(meansq + 1e-06) * norm_gain.astype(jnp.float32)).astype(jnp.bfloat16)
    gate = jnp.dot(normed, gate_weight, preferred_element_type=jnp.float32)
    linear = jnp.dot(normed, linear_weight, preferred_element_type=jnp.float32)
    hidden = (jax.nn.gelu(gate, approximate=True) * linear).astype(jnp.bfloat16)
    return jnp.dot(hidden, output_weight, preferred_element_type=jnp.float32).astype(jnp.bfloat16)
```

```python
import jax
import jax.numpy as jnp
from jax import lax
from jax.sharding import PartitionSpec as P

NAMES = ("zh", "y", "zl", "x", "c")
SIZES = (4, 4, 2, 4, 2)
F32, BF16 = jnp.float32, jnp.bfloat16


def coords():
    for zh in range(4):
        for y in range(4):
            for zl in range(2):
                for x in range(4):
                    for c in range(2):
                        yield zh, y, zl, x, c


def number(zh, y, zl, x, c):
    return (((zh % 4 * 4 + y % 4) * 2 + zl % 2) * 4 + x % 4) * 2 + c % 2


def send(v, move):
    return lax.ppermute(v, NAMES, [(number(*p), number(*move(*p))) for p in coords()])


def to_column(flip):
    def move(zh, y, zl, x, c):
        half = (y & 1) ^ flip
        return zh, 2 * c + half, zl, x, y >> 1

    return move


def ring(zh, y, zl, x, c):
    z = (2 * zh + zl + (1 if c == 0 else -1)) % 8
    return z >> 1, y, z & 1, x, c


def swap(zh, y, zl, x, c):
    return zh, y, zl, x, 1 - c


def quarter(a, b):
    return lambda zh, y, zl, x, c: (zh, y, zl ^ a, x, c ^ b)


def first(k):
    return lambda zh, y, zl, x, c: (zh, y, zl, x + k, c) if c == 0 else (zh, y + k, zl, x, c)


def second(k):
    return lambda zh, y, zl, x, c: (zh, y + k, zl, x, c) if c == 0 else (zh, y, zl, x + k, c)


SHIFTS = (1, 3, 2)
QUARTERS = ((0, 1), (1, 0), (1, 1))


def local(tokens, norm_gain, gate_weight, linear_weight, output_weight):
    zh, y, zl, x, c = (lax.axis_index(n) for n in NAMES)
    z = 2 * zh + zl
    way = 1 - 2 * c
    odd = (y & 1) == 1
    upper = c == 1

    halves = [
        jnp.concatenate((gate_weight[:, s], linear_weight[:, s]), axis=1)
        for s in (slice(0, 320), slice(320, 640))
    ]
    ga = send(jnp.where(odd, halves[1], halves[0]), to_column(0))
    gb = send(jnp.where(odd, halves[0], halves[1]), to_column(1))
    oa = send(jnp.where(odd, output_weight[320:], output_weight[:320]), to_column(0))
    ob = send(jnp.where(odd, output_weight[:320], output_weight[320:]), to_column(1))

    def chip_block(a, b, axis):
        own = jnp.where(odd, jnp.concatenate((b, a), axis), jnp.concatenate((a, b), axis))
        other = send(own, swap)
        return jnp.where(
            upper, jnp.concatenate((other, own), axis), jnp.concatenate((own, other), axis)
        )

    gain_rows = jnp.broadcast_to(norm_gain[None], (8, 256))

    def piece(a, b):
        q = 2 * (zl ^ a) + (c ^ b)
        rows = lax.dynamic_slice_in_dim(tokens, q * 128, 128, 0)
        return jnp.concatenate((rows, gain_rows), axis=0)

    got = {(0, 0): piece(0, 0)}
    for ab in QUARTERS:
        got[ab] = send(piece(*ab), quarter(*ab))
    pair = [
        jnp.where(
            upper,
            jnp.concatenate((got[a, 1], got[a, 0]), 1),
            jnp.concatenate((got[a, 0], got[a, 1]), 1),
        )
        for a in range(2)
    ]
    start = jnp.where(
        zl == 1, jnp.concatenate((pair[1], pair[0]), 1), jnp.concatenate((pair[0], pair[1]), 1)
    )
    line = {0: start}
    for k in SHIFTS:
        line[(-k) % 4] = send(start, first(k))
    line = jnp.stack([line[i] for i in range(4)])
    plane = {0: line}
    for k in SHIFTS:
        plane[(-k) % 4] = send(line, second(k))
    plane = jnp.stack([plane[j] for j in range(4)])
    plane = jnp.where(upper, jnp.swapaxes(plane, 0, 1), plane)
    plane = jnp.roll(plane, x, axis=1)
    values = plane[:, :, :128].astype(F32)
    gain = plane[0, :, 128].astype(F32)[None, :, None]
    meansq = jnp.mean(values * values, axis=(1, 3), keepdims=True)
    normed = (values * lax.rsqrt(meansq + 1e-06) * gain).astype(BF16)
    normed = normed.reshape(4, 4, 128, 2, 512).transpose(0, 2, 3, 1, 4).reshape(512, 4096)

    def columns(source, offset=0, width=1024):
        return lax.dynamic_slice_in_dim(normed, (source % 8 >> 1) * 1024 + offset, width, 1)

    def dot(a, b):
        return jnp.dot(a, b, preferred_element_type=F32)

    mine = chip_block(ga, gb, 0)
    sums = [dot(columns(z), mine), None]
    for k in range(1, 5):
        if k == 4:
            mine = lax.dynamic_slice_in_dim(mine, c * 512, 512, 0)
        mine = send(mine, ring)
        theirs = send(mine, swap)
        if k < 4:
            add = dot(columns(z - way * k), mine) + dot(columns(z + way * k), theirs)
        else:
            add = dot(columns(z + 4, c * 512, 512), mine)
            add += dot(columns(z + 4, (1 - c) * 512, 512), theirs)
        sums[k % 2] = add if sums[k % 2] is None else sums[k % 2] + add
    hidden = jnp.concatenate(
        [
            (jax.nn.gelu(s[:, :320], approximate=True) * s[:, 320:]).astype(BF16)
            for s in sums
        ],
        axis=1,
    )

    block = jnp.zeros((640, 4096), BF16)

    def place(block, part, source, odd_step, offset=0):
        high = source % 8 >> 1
        for s in range(part.shape[1] // 512):
            xs = (high & 1) * 2 + s + offset
            at = (high >> 1) * 2048 + ((xs - x) % 4) * 512
            block = lax.dynamic_update_slice(
                block, part[:, 512 * s : 512 * s + 512], (320 * odd_step, at)
            )
        return block

    mine = chip_block(oa, ob, 1)
    block = place(block, mine, z, 0)
    for k in range(1, 5):
        if k == 4:
            mine = lax.dynamic_slice_in_dim(mine, c * 512, 512, 1)
        mine = send(mine, ring)
        theirs = send(mine, swap)
        if k < 4:
            block = place(block, mine, z - way * k, k % 2)
            block = place(block, theirs, z + way * k, k % 2)
        else:
            block = place(block, mine, z + 4, 0, c)
            block = place(block, theirs, z + 4, 0, 1 - c)

    terms = dot(hidden, block).astype(BF16).reshape(4, 128, 2, 4, 512)

    def part(k):
        return jnp.where(
            upper, terms[k].transpose(2, 0, 1, 3), terms[:, :, :, k]
        ).reshape(512, 1024)

    total = part(0).astype(F32)
    for r in [send(part(k), first(k)) for k in SHIFTS]:
        total += r.astype(F32)
    half = total.astype(BF16).reshape(4, 128, 1024)
    total = total.reshape(4, 128, 1024)[0]
    for r in [send(half[k], second(k)) for k in SHIFTS]:
        total += r.astype(F32)
    done = total.astype(BF16)

    def columns_for(a, b):
        return lax.dynamic_slice_in_dim(done, (2 * (zl ^ a) + (c ^ b)) * 256, 256, 1)

    out = jnp.zeros((512, 256), BF16)
    for a, b in ((0, 0),) + QUARTERS:
        rows = columns_for(a, b)
        if (a, b) != (0, 0):
            rows = send(rows, quarter(a, b))
        out = lax.dynamic_update_slice(out, rows, ((2 * (zl ^ a) + (c ^ b)) * 128, 0))
    return out


def solution(mesh):
    fine = jax.sharding.Mesh(mesh.devices.reshape(SIZES), NAMES)
    row, col = ("zh", "y"), ("zl", "x", "c")
    return jax.shard_map(
        local,
        mesh=fine,
        in_specs=(P(row, col), P(col), P(row, col), P(row, col), P(col, row)),
        out_specs=P(row, col),
        check_vma=False,
    )
```

```python
import jax
import jax.numpy as jnp
from jax import lax
from jax.experimental import pallas as pl
from jax.experimental.pallas import tpu as pltpu
from jax.sharding import PartitionSpec as P

NAMES = ("zh", "y", "zl", "x", "c")
SIZES = (4, 4, 2, 4, 2)
F32, BF16 = jnp.float32, jnp.bfloat16


def coords():
    for zh in range(4):
        for y in range(4):
            for zl in range(2):
                for x in range(4):
                    for c in range(2):
                        yield zh, y, zl, x, c


def number(zh, y, zl, x, c):
    return (((zh % 4 * 4 + y % 4) * 2 + zl % 2) * 4 + x % 4) * 2 + c % 2


def send(v, move):
    return lax.ppermute(v, NAMES, [(number(*p), number(*move(*p))) for p in coords()])


def to_column(flip):
    def move(zh, y, zl, x, c):
        half = (y & 1) ^ flip
        return zh, 2 * c + half, zl, x, y >> 1

    return move


def ring(zh, y, zl, x, c):
    z = (2 * zh + zl + (1 if c == 0 else -1)) % 8
    return z >> 1, y, z & 1, x, c


def swap(zh, y, zl, x, c):
    return zh, y, zl, x, 1 - c


def quarter_in(a, b):
    def move(zh, y, zl, x, c):
        return (zh, y, zl ^ a, x, c ^ b) if c ^ b == 0 else (zh, x, zl ^ a, y, c ^ b)

    return move


def quarter_out(a, b):
    def move(zh, y, zl, x, c):
        return (zh, y, zl ^ a, x, c ^ b) if c == 0 else (zh, x, zl ^ a, y, c ^ b)

    return move


def first(k):
    return lambda zh, y, zl, x, c: (zh, y, zl, x + k, c) if c == 0 else (zh, y + k, zl, x, c)


def second(k):
    return lambda zh, y, zl, x, c: (zh, y + k, zl, x, c) if c == 0 else (zh, y, zl, x + k, c)


SHIFTS = (1, 3, 2)
QUARTERS = ((0, 0), (0, 1), (1, 0), (1, 1))


def norm_kernel(at_ref, gain_ref, r0, r1, r2, r3, out_ref):
    for j, rows in enumerate((r0, r1, r2, r3)):
        values = [rows[i].astype(F32) for i in range(4)]
        squares = sum(jnp.sum(v * v, axis=-1, keepdims=True) for v in values)
        scale = lax.rsqrt(squares * (1 / 4096) + 1e-06)
        for i in range(4):
            n = (values[i] * scale * gain_ref[i : i + 1]).astype(BF16)
            for s in range(2):
                at = pl.multiple_of(at_ref[2 * i + s], 512)
                out_ref[j, :, pl.ds(at, 512)] = n[:, 512 * s : 512 * s + 512]


def norm(at, gain, plane):
    rows = pl.BlockSpec((4, 16, 1024), lambda g, at: (0, g, 0))
    return pl.pallas_call(
        norm_kernel,
        grid_spec=pltpu.PrefetchScalarGridSpec(
            num_scalar_prefetch=1,
            grid=(8,),
            in_specs=[pl.BlockSpec((4, 1024), lambda g, at: (0, 0))] + [rows] * 4,
            out_specs=pl.BlockSpec((4, 16, 4096), lambda g, at: (0, g, 0)),
        ),
        out_shape=jax.ShapeDtypeStruct((4, 128, 4096), BF16),
        cost_estimate=pl.CostEstimate(
            flops=16 * 512 * 4096, bytes_accessed=4 * 512 * 4096, transcendentals=0
        ),
    )(at, gain, *plane).reshape(512, 4096)


def dot(a, b):
    return jnp.dot(a, b, preferred_element_type=F32)


def local(tokens, norm_gain, gate_weight, linear_weight, output_weight):
    zh, y, zl, x, c = (lax.axis_index(n) for n in NAMES)
    z = 2 * zh + zl
    way = 1 - 2 * c
    odd = (y & 1) == 1
    here = jnp.where(c == 0, x, y)

    halves = [
        jnp.concatenate((gate_weight[:, s], linear_weight[:, s]), axis=1)
        for s in (slice(0, 320), slice(320, 640))
    ]
    ga = send(jnp.where(odd, halves[1], halves[0]), to_column(0))
    gb = send(jnp.where(odd, halves[0], halves[1]), to_column(1))

    gain_rows = jnp.broadcast_to(norm_gain[None], (8, 256))
    got = {}
    for a, b in QUARTERS:
        q = 2 * (zl ^ a) + (c ^ b)
        rows = lax.dynamic_slice_in_dim(tokens, q * 128, 128, 0)
        got[a, b] = send(jnp.concatenate((rows, gain_rows), axis=0), quarter_in(a, b))
    oa = send(jnp.where(odd, output_weight[320:], output_weight[:320]), to_column(0))
    ob = send(jnp.where(odd, output_weight[:320], output_weight[320:]), to_column(1))

    def chip_block(a, b, axis):
        own = jnp.where(odd, jnp.concatenate((b, a), axis), jnp.concatenate((a, b), axis))
        return jnp.concatenate((own, send(own, swap)), axis)

    start = jnp.zeros((136, 1024), BF16)
    for a, b in QUARTERS:
        start = lax.dynamic_update_slice(start, got[a, b], (0, (2 * (zl ^ a) + (c ^ b)) * 256))
    line = {0: start}
    for k in SHIFTS:
        line[(-k) % 4] = send(start, first(k))
    line = jnp.stack([line[i] for i in range(4)])
    plane = {0: line}
    for k in SHIFTS:
        plane[(-k) % 4] = send(line, second(k))

    at = []
    for i in range(4):
        for s in range(2):
            xs = (here + i) % 4
            ahead = (2 * s + (xs >> 1) - zh) * way % 4
            place_of = jnp.array([0, 2, 3, 1])[ahead]
            at.append(place_of * 1024 + ((xs & 1) ^ c) * 512)
    normed = norm(
        jnp.stack(at).astype(jnp.int32),
        line[:, 128].astype(F32),
        [plane[j] for j in range(4)],
    )

    def slot(source):
        ahead = ((source % 8 >> 1) - zh) * way % 4
        return jnp.array([0, 2, 3, 1])[ahead]

    mine, theirs = [chip_block(ga, gb, 0)], [None]
    for k in range(1, 5):
        mine.append(send(mine[-1] if k < 4 else mine[-1][:512], ring))
        theirs.append(send(mine[-1], swap))
    uneven = jnp.zeros((4096, 640), BF16)
    for k in (1, 3):
        uneven = lax.dynamic_update_slice(uneven, mine[k], (slot(z - way * k) * 1024, 0))
        base = slot(z + way * k) * 1024
        uneven = lax.dynamic_update_slice(uneven, theirs[k][512:], (base, 0))
        uneven = lax.dynamic_update_slice(uneven, theirs[k][:512], (base + 512, 0))
    even = jnp.concatenate((mine[0], mine[2], theirs[2][512:], theirs[2][:512]), axis=0)
    sums = [
        dot(normed[:, :3072], even)
        + dot(normed[:, 3072:], jnp.concatenate((mine[4], theirs[4]), axis=0)),
        dot(normed, uneven),
    ]
    hidden = jnp.concatenate(
        [
            (jax.nn.gelu(s[:, :320], approximate=True) * s[:, 320:]).astype(BF16)
            for s in sums
        ],
        axis=1,
    )

    block = jnp.zeros((640, 4096), BF16)

    def place(block, part, source, k, flip):
        high = source % 8 >> 1
        for s in range(part.shape[1] // 512):
            xs = (high & 1) * 2 + (s ^ flip)
            to = ((xs - here) % 4) * 1024 + (high >> 1) * 512
            block = lax.dynamic_update_slice(
                block, part[:, 512 * s : 512 * s + 512], (320 * (k % 2), to)
            )
        return block

    mine = chip_block(oa, ob, 1)
    block = place(block, mine, z, 0, c)
    for k in range(1, 5):
        mine = send(mine if k < 4 else mine[:, :512], ring)
        theirs = send(mine, swap)
        block = place(block, mine, z - way * k, k, c)
        block = place(block, theirs, z + way * k, k, 1 - c)

    terms = [dot(hidden, block[:, 1024 * k : 1024 * k + 1024]) for k in (1, 3, 2, 0)]
    total = terms[3]
    for r in [send(t.astype(BF16), first(k)) for t, k in zip(terms, SHIFTS)]:
        total += r.astype(F32)
    half = total.astype(BF16)
    total = total[:128]
    for r in [send(half[128 * k : 128 * k + 128], second(k)) for k in SHIFTS]:
        total += r.astype(F32)
    done = total.astype(BF16)

    out = jnp.zeros((512, 256), BF16)
    for a, b in QUARTERS:
        q = 2 * (zl ^ a) + (c ^ b)
        rows = send(lax.dynamic_slice_in_dim(done, q * 256, 256, 1), quarter_out(a, b))
        out = lax.dynamic_update_slice(out, rows, (q * 128, 0))
    return out


def solution(mesh):
    fine = jax.sharding.Mesh(mesh.devices.reshape(SIZES), NAMES)
    row, col = ("zh", "y"), ("zl", "x", "c")
    return jax.shard_map(
        local,
        mesh=fine,
        in_specs=(P(row, col), P(col), P(row, col), P(row, col), P(col, row)),
        out_specs=P(row, col),
        check_vma=False,
    )
```
